32 devices in a mesh: row: 8 (over y, x, core), col: 4 (over z).
Axes of the slice: x: 2, y: 2, z: 4, core: 2. Of those that a mesh axis runs over, the one named last changes fastest.
Arguments:
- density_start: float32 [512, 512], P('row', 'col'), may hold values from -0.5 to 1, as said below
- branches: int32 [6], replicated, may hold values from 0 to 1, as said below
Outputs:
- density: float32 [512, 512], P('row', 'col')
- occupations: float32 [6, 2], replicated
The draws below stay inside these ranges and needn't reach their ends.
Inputs may be any that keep to these rules, and one draw needn't show every extreme that they name: density_start is symmetric with eigenvalues inside 0 to 1. `branches`: each entry is 0 or 1, and exactly 3 entries are 1.
All inputs are finite; a program needn't handle non-finite values.
Results may differ from the reference program's by a relative error of at most 0.0025.
Values may be sent and summed in bfloat16 or wider, within the bound.
A program may use at most 64 MiB of HBM per device.

```python
import jax
import jax.numpy as jnp

ITERS = 6
N = 512


def draw_density_start(key, part):
    samples = jnp.clip(jax.random.normal(key, (N, N), jnp.float32), -6.0, 6.0)
    symmetric = (samples + samples.T) / (2.0 * jnp.sqrt(2.0 * N))
    return 0.5 * jnp.eye(N, dtype=jnp.float32) + 0.45 * symmetric


def draw_branches(key, part):
    return (jax.random.permutation(key, ITERS) % 2).astype(jnp.int32)


def setup_inputs(seed: int = 0) -> dict:
    keys = jax.random.split(jax.random.key(seed), 3)
    density_start = draw_density_start(jax.random.fold_in(keys[2], 71), 0)
    branches = draw_branches(jax.random.fold_in(keys[2], 71), 0)
    return dict(density_start=density_start, branches=branches)


def reference(density_start, branches):
    density = density_start
    records = []
    for iteration in range(ITERS):
        narrow = density.astype(jnp.bfloat16)
        square = jnp.dot(narrow, narrow, preferred_element_type=jnp.float32)
        records.append(jnp.stack([jnp.trace(density), jnp.trace(square)]) / N)
        density = jnp.where(branches[iteration] == 1, 2.0 * density - square, square)
    return density, jnp.stack(records)
```

```python
import functools

import jax
import jax.numpy as jnp
from jax import lax
from jax.experimental import pallas as pl
from jax.experimental.pallas import tpu as pltpu
from jax.sharding import PartitionSpec as P

ITERS = 6


def diagonal_sum(square, first):
    rows, cols = square.shape
    row_ids = lax.broadcasted_iota(jnp.int32, (rows, cols), 0)
    col_ids = lax.broadcasted_iota(jnp.int32, (rows, cols), 1)
    return jnp.sum(jnp.where(row_ids == col_ids + first, square, 0.0), keepdims=True)


def purify(x, b, branches, rows_here, cols_here, density_ref, occupations_ref):
    size = x.shape[0]
    tile = min(256, size)
    tiles = size // tile
    row_first = pl.multiple_of(lax.axis_index("row") * rows_here, rows_here)
    col_first = pl.multiple_of(lax.axis_index("col") * cols_here, cols_here)
    trace = jnp.zeros((1, 1), jnp.float32)
    for t in range(tiles):
        ids = slice(t * tile, (t + 1) * tile)
        trace = trace + diagonal_sum(x[ids, ids], 0)
        b[0, :, ids] = x[:, ids].astype(jnp.bfloat16)
    records = []
    for iteration in range(ITERS):
        now, later = iteration % 2, (iteration + 1) % 2
        one = branches[iteration] == 1
        keep = jnp.where(one, 2.0, 0.0)
        sign = jnp.where(one, -1.0, 1.0)
        square_trace = jnp.zeros((1, 1), jnp.float32)
        if iteration < ITERS - 1:
            for t in range(tiles):
                ids = slice(t * tile, (t + 1) * tile)
                square = jnp.dot(b[now], b[now, :, ids], preferred_element_type=jnp.float32)
                square_trace = square_trace + diagonal_sum(square[ids, :], 0)
                fresh = keep * x[:, ids] + sign * square
                x[:, ids] = fresh
                b[later, :, ids] = fresh.astype(jnp.bfloat16)
        else:
            for t in range(tiles):
                ids = slice(t * tile, (t + 1) * tile)
                part = b[now, :, ids].astype(jnp.float32)
                square_trace = square_trace + jnp.sum(part * part, keepdims=True)
            square = jnp.dot(
                b[now, pl.ds(row_first, rows_here), :],
                b[now, :, pl.ds(col_first, cols_here)],
                preferred_element_type=jnp.float32,
            )
            mine = x[pl.ds(row_first, rows_here), pl.ds(col_first, cols_here)]
            density_ref[...] = keep * mine + sign * square
        records.append((trace, square_trace))
        trace = keep * trace + sign * square_trace
    shape = occupations_ref.shape
    row_ids = lax.broadcasted_iota(jnp.int32, shape, 0)
    col_ids = lax.broadcasted_iota(jnp.int32, shape, 1)
    out = jnp.zeros(shape, jnp.float32)
    for k, pair in enumerate(records):
        for j, value in enumerate(pair):
            out = jnp.where((row_ids == k) & (col_ids == j), value / size, out)
    occupations_ref[...] = out


def compute_kernel(rows_here, cols_here, branches, start, density_ref, occupations_ref, x, b):
    x[...] = start[...]
    purify(x, b, branches, rows_here, cols_here, density_ref, occupations_ref)


def body(density_start, branches):
    rows_here, cols_here = density_start.shape
    size = cols_here * lax.axis_size("col")
    whole = lax.all_gather(density_start, "col", axis=1, tiled=True)
    whole = lax.all_gather(whole, "row", axis=0, tiled=True)
    return pl.pallas_call(
        functools.partial(compute_kernel, rows_here, cols_here),
        out_shape=(
            jax.ShapeDtypeStruct((rows_here, cols_here), jnp.float32),
            jax.ShapeDtypeStruct((ITERS, 2), jnp.float32),
        ),
        in_specs=[
            pl.BlockSpec(memory_space=pltpu.SMEM),
            pl.BlockSpec(memory_space=pltpu.VMEM),
        ],
        out_specs=(
            pl.BlockSpec(memory_space=pltpu.VMEM),
            pl.BlockSpec(memory_space=pltpu.VMEM),
        ),
        scratch_shapes=[
            pltpu.VMEM((size, size), jnp.float32),
            pltpu.VMEM((2, size, size), jnp.bfloat16),
        ],
    )(branches, whole)


def solution(mesh):
    in_specs = (P("row", "col"), P())
    out_specs = (P("row", "col"), P())
    return jax.shard_map(body, mesh=mesh, in_specs=in_specs, out_specs=out_specs, check_vma=False)
```

```python
import functools

import jax
import jax.numpy as jnp
from jax import lax
from jax.experimental import pallas as pl
from jax.experimental.pallas import tpu as pltpu
from jax.sharding import PartitionSpec as P

ITERS = 6


def diagonal_sum(square, first):
    rows, cols = square.shape
    row_ids = lax.broadcasted_iota(jnp.int32, (rows, cols), 0)
    col_ids = lax.broadcasted_iota(jnp.int32, (rows, cols), 1)
    return jnp.sum(jnp.where(row_ids == col_ids + first, square, 0.0), keepdims=True)


def purify(x, b, branches, rows_here, cols_here, density_ref, occupations_ref):
    size = x.shape[0]
    tile = min(256, size)
    tiles = size // tile
    row_first = pl.multiple_of(lax.axis_index("row") * rows_here, rows_here)
    col_first = pl.multiple_of(lax.axis_index("col") * cols_here, cols_here)
    trace = jnp.zeros((1, 1), jnp.float32)
    for t in range(tiles):
        ids = slice(t * tile, (t + 1) * tile)
        trace = trace + diagonal_sum(x[ids, ids], 0)
        b[0, :, ids] = x[:, ids].astype(jnp.bfloat16)
    records = []
    for iteration in range(ITERS):
        now, later = iteration % 2, (iteration + 1) % 2
        one = branches[iteration] == 1
        keep = jnp.where(one, 2.0, 0.0)
        sign = jnp.where(one, -1.0, 1.0)
        square_trace = jnp.zeros((1, 1), jnp.float32)
        if iteration < ITERS - 1:
            for t in range(tiles):
                ids = slice(t * tile, (t + 1) * tile)
                square = jnp.dot(b[now], b[now, :, ids], preferred_element_type=jnp.float32)
                square_trace = square_trace + diagonal_sum(square[ids, :], 0)
                fresh = keep * x[:, ids] + sign * square
                x[:, ids] = fresh
                b[later, :, ids] = fresh.astype(jnp.bfloat16)
        else:
            for t in range(tiles):
                ids = slice(t * tile, (t + 1) * tile)
                part = b[now, :, ids].astype(jnp.float32)
                square_trace = square_trace + jnp.sum(part * part, keepdims=True)
            square = jnp.dot(
                b[now, pl.ds(row_first, rows_here), :],
                b[now, :, pl.ds(col_first, cols_here)],
                preferred_element_type=jnp.float32,
            )
            mine = x[pl.ds(row_first, rows_here), pl.ds(col_first, cols_here)]
            density_ref[...] = keep * mine + sign * square
        records.append((trace, square_trace))
        trace = keep * trace + sign * square_trace
    shape = occupations_ref.shape
    row_ids = lax.broadcasted_iota(jnp.int32, shape, 0)
    col_ids = lax.broadcasted_iota(jnp.int32, shape, 1)
    out = jnp.zeros(shape, jnp.float32)
    for k, pair in enumerate(records):
        for j, value in enumerate(pair):
            out = jnp.where((row_ids == k) & (col_ids == j), value / size, out)
    occupations_ref[...] = out

MESH = pl.DeviceIdType.MESH


def xor_fixed(index, bits, fixed):
    out = 0
    for bit in range(bits):
        digit = lax.rem(lax.div(index, 1 << bit), 2)
        out = out + ((1 - digit) if (fixed >> bit) & 1 else digit) * (1 << bit)
    return out


def xor_traced(left, right, bits):
    out = 0
    for bit in range(bits):
        a = lax.rem(lax.div(left, 1 << bit), 2)
        b = lax.rem(lax.div(right, 1 << bit), 2)
        out = out + (a + b - 2 * a * b) * (1 << bit)
    return out


def relay_slots(tiles):
    slots = [(d, 0) for d in range(1, tiles)]
    for a in range(1, tiles):
        for b in range(a + 1, tiles):
            d = min((bin(v).count("1"), v) for v in (a, b))[1]
            slots.append((d, a ^ b))
    return slots


def whole_kernel(tiles, halves, slots, branches, start, density_ref, occupations_ref,
                 x, b, local_sem, line_send, line_recv, relay_send, relay_recv, peer_send, peer_recv):
    rows_here, cols_here = density_ref.shape
    bits = tiles.bit_length() - 1
    row, col = lax.axis_index("row"), lax.axis_index("col")
    band, half = lax.div(row, halves), lax.rem(row, halves)

    def block(band_at, col_at):
        first = pl.multiple_of((band_at * halves + half) * rows_here, rows_here)
        return x.at[pl.ds(first, rows_here), pl.ds(pl.multiple_of(col_at * cols_here, cols_here), cols_here)]

    def tile(band_at, col_at):
        side = cols_here
        return (pl.ds(pl.multiple_of(band_at * side, side), side),
                pl.ds(pl.multiple_of(col_at * side, side), side))

    own = pltpu.make_async_copy(start, block(band, col), local_sem)
    own.start()

    cols = [xor_fixed(col, bits, k) for k in range(tiles)]
    bands = [xor_fixed(band, bits, d) for d in range(tiles)]
    peers = [band * halves + lax.rem(half + s, halves) for s in range(1, halves)]
    partners = [(row, cols[k]) for k in range(1, tiles)]
    partners += [(bands[d] * halves + half, col) for d in range(1, tiles)]
    partners += [(p, col) for p in peers]
    barrier = pltpu.get_barrier_semaphore()
    for partner in partners:
        pl.semaphore_signal(barrier, inc=1, device_id=partner, device_id_type=MESH)
    pl.semaphore_wait(barrier, len(partners))
    own.wait()

    def send(ref, send_sem, recv_sem, device):
        return pltpu.make_async_remote_copy(
            src_ref=ref, dst_ref=ref, send_sem=send_sem, recv_sem=recv_sem,
            device_id=device, device_id_type=MESH,
        )

    line = {k: send(block(band, col), line_send.at[k], line_recv.at[k], (row, cols[k]))
            for k in range(1, tiles)}
    relay = [send(block(band, bands[e]), relay_send.at[i], relay_recv.at[i], (bands[d] * halves + half, col))
             for i, (d, e) in enumerate(slots)]
    held = [block(band, cols[k]) for k in range(tiles)]
    held += [block(bands[d], bands[d ^ e]) for d, e in slots]
    peer = [[send(ref, peer_send.at[s, i], peer_recv.at[s, i], (p, col)) for s, p in enumerate(peers)]
            for i, ref in enumerate(held)]

    for k in range(1, tiles):
        line[k].start()
    for k in range(tiles):
        if k:
            line[k].wait_recv()
        here = xor_traced(band, cols[k], bits)
        for e in range(tiles):
            @pl.when(here == e)
            def _():
                for i, slot in enumerate(slots):
                    if slot[1] == e:
                        relay[i].start()
        for copy in peer[k]:
            copy.start()
    for i in range(len(slots)):
        relay[i].wait_recv()
        for copy in peer[tiles + i]:
            copy.start()
    for k in range(tiles):
        for copy in peer[k]:
            copy.wait_recv()
    for e in range(1, tiles):
        x[tile(bands[e], band)] = x[tile(band, bands[e])].T
    for i, (d, e) in enumerate(slots):
        for copy in peer[tiles + i]:
            copy.wait_recv()
        if e:
            x[tile(bands[d ^ e], bands[d])] = x[tile(bands[d], bands[d ^ e])].T
    for copy in list(line.values()) + relay + [c for group in peer for c in group]:
        copy.wait_send()
    purify(x, b, branches, rows_here, cols_here, density_ref, occupations_ref)


def body(density_start, branches):
    rows_here, cols_here = density_start.shape
    tiles = lax.axis_size("col")
    halves = lax.axis_size("row") // tiles
    assert tiles & (tiles - 1) == 0 and halves * rows_here == cols_here
    size = cols_here * tiles
    slots = relay_slots(tiles)
    dma = pltpu.SemaphoreType.DMA
    return pl.pallas_call(
        functools.partial(whole_kernel, tiles, halves, slots),
        out_shape=(
            jax.ShapeDtypeStruct((rows_here, cols_here), jnp.float32),
            jax.ShapeDtypeStruct((ITERS, 2), jnp.float32),
        ),
        in_specs=[
            pl.BlockSpec(memory_space=pltpu.SMEM),
            pl.BlockSpec(memory_space=pl.ANY),
        ],
        out_specs=(
            pl.BlockSpec(memory_space=pltpu.VMEM),
            pl.BlockSpec(memory_space=pltpu.VMEM),
        ),
        scratch_shapes=[
            pltpu.VMEM((size, size), jnp.float32),
            pltpu.VMEM((2, size, size), jnp.bfloat16),
            dma,
            dma((tiles,)),
            dma((tiles,)),
            dma((len(slots),)),
            dma((len(slots),)),
            dma((halves - 1, tiles + len(slots))),
            dma((halves - 1, tiles + len(slots))),
        ],
        compiler_params=pltpu.CompilerParams(collective_id=0, has_side_effects=True),
    )(branches, density_start)


def solution(mesh):
    in_specs = (P("row", "col"), P())
    out_specs = (P("row", "col"), P())
    return jax.shard_map(body, mesh=mesh, in_specs=in_specs, out_specs=out_specs, check_vma=False)
```
